32 devices in a mesh: row: 4 (over z), col: 8 (over y, x, core).
Axes of the slice: x: 2, y: 2, z: 4, core: 2. Of those that a mesh axis runs over, the one named last changes fastest.
Arguments:
- tokens: bfloat16 [1024, 8192], P('row', 'col'), may hold values from -6 to 6
- gate_frozen_weight: bfloat16 [8192, 28672], P('col', 'row'), may hold values from -0.0625 to 0.0625
- gate_left_factor: bfloat16 [8192, 64], P('col'), may hold values from -0.046875 to 0.046875
- gate_right_factor: bfloat16 [64, 28672], P(None, 'row'), may hold values from -0.75 to 0.75
- gate_column_magnitude: float32 [28672], P('row'), may hold values from 0.5 to 1.5
- up_frozen_weight: bfloat16 [8192, 28672], P('col', 'row'), may hold values from -0.0625 to 0.0625
- up_left_factor: bfloat16 [8192, 64], P('col'), may hold values from -0.046875 to 0.046875
- up_right_factor: bfloat16 [64, 28672], P(None, 'row'), may hold values from -0.75 to 0.75
- up_column_magnitude: float32 [28672], P('row'), may hold values from 0.5 to 1.5
- down_frozen_weight: bfloat16 [28672, 8192], P('row', 'col'), may hold values from -0.03125 to 0.03125
- down_left_factor: bfloat16 [28672, 64], P('row'), may hold values from -0.02734375 to 0.02734375
- down_right_factor: bfloat16 [64, 8192], P(None, 'col'), may hold values from -0.75 to 0.75
- down_column_magnitude: float32 [8192], P('col'), may hold values from 0.5 to 1.5
Outputs:
- mixed: bfloat16 [1024, 8192], P('row', 'col')
The draws below stay inside these ranges and needn't reach their ends.
All inputs are finite; a program needn't handle non-finite values.
Results may differ from the reference program's by a relative error of at most 0.028.
Values may be sent and summed in bfloat16 or wider, within the bound.
A program may use at most 192 MiB of HBM per device.

```python
import jax
import jax.numpy as jnp
from jax import lax

MODEL_WIDTH = 8192
HIDDEN_UNITS = 28672
UPDATE_RANK = 64
TOKENS = 1024
N_ROW = 4
N_COL = 8


def block_levels(own_key, shape, cuts, least, largest):
    def one(axis_at, parts):
        draws = jax.random.uniform(jax.random.fold_in(jax.random.fold_in(own_key, 6), axis_at), (parts,), jnp.float32, least / len(cuts), largest / len(cuts))
        return jnp.repeat(jnp.exp(draws), shape[axis_at] // parts).reshape((-1,) + (1,) * (len(shape) - axis_at - 1))

    loudness = one(*cuts[0])
    for cut in cuts[1:]:
        loudness = loudness * one(*cut)
    return loudness


def normal_values(own_key, shape, deviation, bound, cuts=(), kind=jnp.bfloat16):
    result = deviation * jax.random.normal(own_key, shape, jnp.float32)
    if cuts:
        result = result * block_levels(own_key, shape, cuts, -0.22, 0.18)
    return jnp.clip(result, -bound, bound).astype(kind)


def setup_inputs(seed: int = 0) -> dict:
    keys = jax.random.split(jax.random.key(seed), 14)
    tokens = normal_values(keys[0], (TOKENS, MODEL_WIDTH), 1.0, 6.0, ((0, 4), (1, 8)))
    gate_frozen_weight = normal_values(keys[1], (MODEL_WIDTH, HIDDEN_UNITS), MODEL_WIDTH ** -0.5, 0.0625, ((0, 8), (1, 4)))
    gate_left_factor = normal_values(keys[2], (MODEL_WIDTH, UPDATE_RANK), (0.3 * MODEL_WIDTH ** -0.5), 0.046875, ((0, 8),))
    gate_right_factor = normal_values(keys[3], (UPDATE_RANK, HIDDEN_UNITS), UPDATE_RANK ** -0.5, 0.75, ((1, 4),))
    gate_column_magnitude = jnp.clip(1.0 + 0.1 * jax.random.normal(keys[4], (HIDDEN_UNITS,), jnp.float32), 0.5, 1.5)
    up_frozen_weight = normal_values(keys[5], (MODEL_WIDTH, HIDDEN_UNITS), MODEL_WIDTH ** -0.5, 0.0625, ((0, 8), (1, 4)))
    up_left_factor = normal_values(keys[6], (MODEL_WIDTH, UPDATE_RANK), (0.3 * MODEL_WIDTH ** -0.5), 0.046875, ((0, 8),))
    up_right_factor = normal_values(keys[7], (UPDATE_RANK, HIDDEN_UNITS), UPDATE_RANK ** -0.5, 0.75, ((1, 4),))
    up_column_magnitude = jnp.clip(1.0 + 0.1 * jax.random.normal(keys[8], (HIDDEN_UNITS,), jnp.float32), 0.5, 1.5)
    down_frozen_weight = normal_values(keys[9], (HIDDEN_UNITS, MODEL_WIDTH), HIDDEN_UNITS ** -0.5, 0.03125, ((0, 4), (1, 8)))
    down_left_factor = normal_values(keys[10], (HIDDEN_UNITS, UPDATE_RANK), (0.3 * HIDDEN_UNITS ** -0.5), 0.02734375, ((0, 4),))
    down_right_factor = normal_values(keys[11], (UPDATE_RANK, MODEL_WIDTH), UPDATE_RANK ** -0.5, 0.75, ((1, 8),))
    down_column_magnitude = jnp.clip(1.0 + 0.1 * jax.random.normal(keys[12], (MODEL_WIDTH,), jnp.float32), 0.5, 1.5)
    return dict(tokens=tokens, gate_frozen_weight=gate_frozen_weight, gate_left_factor=gate_left_factor, gate_right_factor=gate_right_factor, gate_column_magnitude=gate_column_magnitude, up_frozen_weight=up_frozen_weight, up_left_factor=up_left_factor, up_right_factor=up_right_factor, up_column_magnitude=up_column_magnitude, down_frozen_weight=down_frozen_weight, down_left_factor=down_left_factor, down_right_factor=down_right_factor, down_column_magnitude=down_column_magnitude)


stability_offset = 1e-06

def column_square_totals(weight, low_b, low_a, blocks):
    height, width = weight.shape
    piece = width // blocks
    weight_blocks = weight.reshape(height, blocks, piece).transpose(1, 0, 2)
    factor_blocks = low_a.reshape(low_a.shape[0], blocks, piece).transpose(1, 0, 2)

    def single(pair):
        merged = pair[0].astype(jnp.float32) + jnp.dot(low_b, pair[1], preferred_element_type=jnp.float32)
        return lax.optimization_barrier(jnp.sum(merged * merged, axis=0))
    return lax.map(single, (weight_blocks, factor_blocks)).reshape(width)

def blocked_direct(inputs, weight, blocks):
    piece = inputs.shape[1] // blocks

    def step(index, total):
        start = (index * piece).astype(jnp.int32)
        left = lax.dynamic_slice_in_dim(inputs, start, piece, 1)
        right = lax.dynamic_slice_in_dim(weight, start, piece, 0)
        rounded = jnp.dot(left, right, preferred_element_type=jnp.float32).astype(jnp.bfloat16)
        rounded = lax.optimization_barrier(rounded)
        return total + rounded.astype(jnp.float32)
    start_total = jnp.zeros((inputs.shape[0], weight.shape[1]), jnp.float32)
    return lax.fori_loop(0, blocks, step, start_total)

def adapted_input(inputs, weight, low_b, low_a, scale):
    direct = blocked_direct(inputs, weight, N_COL)
    coords = jnp.dot(inputs, low_b, preferred_element_type=jnp.float32)
    update = jnp.dot(coords, low_a.astype(jnp.float32), precision=lax.Precision.HIGHEST)
    return (direct + update) * scale[None, :]

def adapted_matrix(inputs, weight, low_b, low_a, scale):
    direct = jnp.dot(inputs, weight, preferred_element_type=jnp.float32)
    coords = jnp.dot(inputs, low_b, preferred_element_type=jnp.float32)
    update = jnp.dot(coords, low_a.astype(jnp.float32), precision=lax.Precision.HIGHEST)
    return (direct + update) * scale[None, :]

def reference(tokens, gate_frozen_weight, gate_left_factor, gate_right_factor, gate_column_magnitude, up_frozen_weight, up_left_factor, up_right_factor, up_column_magnitude, down_frozen_weight, down_left_factor, down_right_factor, down_column_magnitude):
    gate_column_scale = gate_column_magnitude / jnp.sqrt(column_square_totals(gate_frozen_weight, gate_left_factor, gate_right_factor, N_ROW) + stability_offset)
    up_column_scale = up_column_magnitude / jnp.sqrt(column_square_totals(up_frozen_weight, up_left_factor, up_right_factor, N_ROW) + stability_offset)
    down_column_scale = down_column_magnitude / jnp.sqrt(column_square_totals(down_frozen_weight, down_left_factor, down_right_factor, N_COL) + stability_offset)
    gate_preactivation = adapted_input(tokens, gate_frozen_weight, gate_left_factor, gate_right_factor, gate_column_scale)
    up_preactivation = adapted_input(tokens, up_frozen_weight, up_left_factor, up_right_factor, up_column_scale)
    hidden_values = (jax.nn.silu(gate_preactivation) * up_preactivation).astype(jnp.bfloat16)
    mixed = adapted_matrix(hidden_values, down_frozen_weight, down_left_factor, down_right_factor, down_column_scale)
    return mixed.astype(jnp.bfloat16)
```

```python
import jax
import jax.numpy as jnp
from jax import lax
from jax.experimental import pallas as pl
from jax.experimental.pallas import tpu as pltpu
from jax.sharding import PartitionSpec as P


stability_offset = 1e-06
chunk_count = 4
F32, BF16 = jnp.float32, jnp.bfloat16


def column_square_totals(weight, low_b, low_a):
    merged = weight.astype(F32) + jnp.dot(low_b, low_a, preferred_element_type=F32)
    return jnp.sum(merged * merged, axis=0)


def swap(value, axis, size, bit):
    return lax.ppermute(value, axis, [(i, i ^ (1 << bit)) for i in range(size)])


def shift(value, axis, size, by):
    return lax.ppermute(value, axis, [(i, (i + by) % size) for i in range(size)])


def butterfly_sum(value, axis, size):
    for bit in range(size.bit_length() - 1):
        value = value + swap(value, axis, size, bit)
    return value


def gather_rows(block, axis, size):
    found = {0: block}
    right, left = block, block
    for step in range(1, size // 2 + 1):
        if 2 * step == size:
            half = block.shape[0] // 2
            first = shift(right[:half], axis, size, 1)
            second = shift(left[half:], axis, size, -1)
            found[step] = jnp.concatenate([first, second], axis=0)
        else:
            right, left = shift(right, axis, size, 1), shift(left, axis, size, -1)
            found[step], found[size - step] = right, left
    return [found[i] for i in range(size)]


def scatter_sum(blocks, axis, size):
    far = size // 2
    half = blocks[0].shape[0] // 2
    right = blocks[far][:half]
    left = blocks[far][half:]
    for step in range(far, 1, -1):
        right = shift(right, axis, size, 1).astype(F32)
        left = shift(left, axis, size, -1).astype(F32)
        if step == far:
            right = jnp.concatenate([right, jnp.zeros_like(right)], axis=0)
            left = jnp.concatenate([jnp.zeros_like(left), left], axis=0)
        right = (right + blocks[step - 1].astype(F32)).astype(BF16)
        left = (left + blocks[size - step + 1].astype(F32)).astype(BF16)
    right = shift(right, axis, size, 1).astype(F32)
    left = shift(left, axis, size, -1).astype(F32)
    return blocks[0].astype(F32) + right + left


def product_kernel(x_ref, cg_ref, cu_ref, wg_ref, rg_ref, wu_ref, ru_ref, sg, su, kg, ku):
    half = sg.shape[0]
    for w, r, c, s, k in ((wg_ref, rg_ref, cg_ref, sg, kg), (wu_ref, ru_ref, cu_ref, su, ku)):
        total = jnp.dot(x_ref[...], w[...], preferred_element_type=F32)
        total += jnp.dot(c[...], r[...], preferred_element_type=F32)
        k[...] = total[:half].astype(BF16)
        s[...] = total[half:].astype(BF16)


def products(x, cg, cu, wg, rg, wu, ru, chunk, width):
    rows, depth = x.shape
    rank = rg.shape[0]
    tile = next(t for t in (256, 128) if width % t == 0)
    steps = width // tile
    first = chunk * steps
    whole = lambda a: pl.BlockSpec(a.shape, lambda j: (0, 0))
    col = lambda height: pl.BlockSpec((height, tile), lambda j: (0, first + j))
    out = pl.BlockSpec((rows // 2, tile), lambda j: (0, j))
    return pl.pallas_call(
        product_kernel,
        grid=(steps,),
        in_specs=[whole(x), whole(cg), whole(cu), col(depth), col(rank), col(depth), col(rank)],
        out_specs=[out] * 4,
        out_shape=[jax.ShapeDtypeStruct((rows // 2, width), BF16)] * 4,
        cost_estimate=pl.CostEstimate(
            flops=4 * rows * (depth + 4 * rank) * width,
            bytes_accessed=4 * (depth + 2 * rows) * width,
            transcendentals=0,
        ),
        compiler_params=pltpu.CompilerParams(vmem_limit_bytes=48 * 1024 * 1024),
    )(x, cg, cu, wg, rg, wu, ru)


def merge_kernel(w_ref, l_ref, r_ref, merged_ref, squares_ref):
    merged = w_ref[...].astype(F32)
    merged += jnp.dot(l_ref[...], r_ref[...], preferred_element_type=F32)
    merged_ref[...] = merged.astype(BF16)

    @pl.when(pl.program_id(0) == 0)
    def _():
        squares_ref[...] = jnp.zeros_like(squares_ref)

    squares_ref[...] += jnp.sum(merged * merged, axis=0, keepdims=True)


def merge(weight, left, right):
    rows, cols = weight.shape
    rank = left.shape[1]
    tile = next(t for t in (512, 256, 128) if rows % t == 0)
    return pl.pallas_call(
        merge_kernel,
        grid=(rows // tile,),
        in_specs=[
            pl.BlockSpec((tile, cols), lambda i: (i, 0)),
            pl.BlockSpec((tile, rank), lambda i: (i, 0)),
            pl.BlockSpec((rank, cols), lambda i: (0, 0)),
        ],
        out_specs=[
            pl.BlockSpec((tile, cols), lambda i: (i, 0)),
            pl.BlockSpec((1, cols), lambda i: (0, 0)),
        ],
        out_shape=[
            jax.ShapeDtypeStruct((rows, cols), BF16),
            jax.ShapeDtypeStruct((1, cols), F32),
        ],
        cost_estimate=pl.CostEstimate(
            flops=8 * rank * rows * cols,
            bytes_accessed=4 * rows * cols,
            transcendentals=0,
        ),
        compiler_params=pltpu.CompilerParams(vmem_limit_bytes=32 * 1024 * 1024),
    )(weight, left, right)


def add(a, b):
    return (a.astype(F32) + b.astype(F32)).astype(BF16)


def shards(
    n_row,
    n_col,
    tokens,
    gate_frozen_weight,
    gate_left_factor,
    gate_right_factor,
    gate_column_magnitude,
    up_frozen_weight,
    up_left_factor,
    up_right_factor,
    up_column_magnitude,
    down_frozen_weight,
    down_left_factor,
    down_right_factor,
    down_column_magnitude,
):
    me_row, me_col = lax.axis_index("row"), lax.axis_index("col")
    bits = n_col.bit_length() - 1
    chains = [list(range(1, bits)), list(range(bits - 1, 0, -1))]

    by_distance = jnp.stack(gather_rows(tokens, "row", n_row))
    own_rows = tokens.shape[0]
    total_rows = own_rows * n_row
    unit = total_rows // n_col // 2

    gate_sq = column_square_totals(gate_frozen_weight, gate_left_factor, gate_right_factor)
    up_sq = column_square_totals(up_frozen_weight, up_left_factor, up_right_factor)
    squares = butterfly_sum(jnp.stack([gate_sq, up_sq]), "col", n_col)
    gate_scale = gate_column_magnitude / jnp.sqrt(squares[0] + stability_offset)
    up_scale = up_column_magnitude / jnp.sqrt(squares[1] + stability_offset)
    down_merged, down_sq = merge(down_frozen_weight, down_left_factor, down_right_factor)
    down_sq = butterfly_sum(down_sq, "row", n_row)
    down_scale = down_column_magnitude / jnp.sqrt(down_sq[0] + stability_offset)

    order = []
    for low in (0, 1):
        for which, chain in enumerate(chains):
            for index in range(1 << (bits - 1)):
                position = low
                for place, bit in enumerate(chain):
                    if index >> (len(chain) - 1 - place) & 1:
                        position |= 1 << bit
                order.append((position, which))

    def start_of(position, which):
        return ((position ^ me_col) * 2 + which) * unit

    pieces = []
    for position, which in order:
        start = start_of(position, which)
        distance = lax.rem(me_row - start // own_rows + n_row, n_row)
        pieces.append(
            lax.dynamic_slice(
                by_distance,
                (distance, lax.rem(start, own_rows), 0),
                (1, unit, tokens.shape[1]),
            )[0]
        )
    x = jnp.concatenate(pieces, axis=0)
    gate_coords = jnp.dot(x, gate_left_factor, preferred_element_type=F32).astype(BF16)
    up_coords = jnp.dot(x, up_left_factor, preferred_element_type=F32).astype(BF16)

    hidden_units = gate_frozen_weight.shape[1]
    width = hidden_units // chunk_count
    group = unit << (bits - 1)
    low_total = [0.0, 0.0]
    for chunk in range(chunk_count):
        cols = slice(chunk * width, (chunk + 1) * width)
        send_g, send_u, keep_g, keep_u = products(
            x, gate_coords, up_coords,
            gate_frozen_weight, gate_right_factor, up_frozen_weight, up_right_factor,
            chunk, width,
        )
        got_g, got_u = swap(send_g, "col", n_col, 0), swap(send_u, "col", n_col, 0)
        states = []
        for which in (0, 1):
            base = which * group
            states.append(
                [(k[base : base + group], g[base : base + group])
                 for k, g in ((keep_g, got_g), (keep_u, got_u))]
            )
        half = group
        for place in range(bits - 1):
            half //= 2
            for which in (0, 1):
                sums = states[which]
                sends = [add(k[half:], g[half:]) for k, g in sums]
                sends = lax.optimization_barrier(tuple(sends))
                keeps = [add(k[:half], g[:half]) for k, g in sums]
                states[which] = [
                    (k, swap(s, "col", n_col, chains[which][place]))
                    for k, s in zip(keeps, sends)
                ]
        parts = []
        for which in (0, 1):
            gate, up = [k.astype(F32) + g.astype(F32) for k, g in states[which]]
            parts.append(
                (
                    jax.nn.silu(gate * gate_scale[None, cols]) * (up * up_scale[None, cols])
                ).astype(BF16)
            )
        for step in range(bits - 1):
            for which in (0, 1):
                other = swap(parts[which], "col", n_col, chains[which][bits - 2 - step])
                parts[which] = jnp.concatenate([parts[which], other], axis=0)
        near = jnp.concatenate(parts, axis=0)
        far = swap(near, "col", n_col, 0)
        for low, hidden in enumerate((near, far)):
            low_total[low] = low_total[low] + jnp.dot(
                hidden, down_merged[cols], preferred_element_type=F32
            )

    mixed = jnp.concatenate(low_total, axis=0).astype(BF16)

    def place_of(owner, which):
        position = owner ^ me_col
        index = 0
        chain = chains[which]
        for place, bit in enumerate(chain):
            index = index + (((position >> bit) & 1) << (len(chain) - 1 - place))
        return (((position & 1) * 2 + which) * (1 << (bits - 1)) + index) * unit

    blocks = []
    for distance in range(n_row):
        target = lax.rem(me_row + distance, n_row)
        rows = []
        for i in range(own_rows // unit):
            number = target * (own_rows // unit) + i
            owner, which = number // 2, i % 2
            rows.append(
                lax.dynamic_slice_in_dim(mixed, place_of(owner, which), unit, 0)
            )
        blocks.append(jnp.concatenate(rows, axis=0))
    total = scatter_sum(blocks, "row", n_row)
    return (total * down_scale[None, :]).astype(BF16)


def solution(mesh):
    placed = (
        P("row", "col"),
        P("col", "row"),
        P("col", None),
        P(None, "row"),
        P("row"),
        P("col", "row"),
        P("col", None),
        P(None, "row"),
        P("row"),
        P("row", "col"),
        P("row", None),
        P(None, "col"),
        P("col"),
    )

    def body(*arrays):
        return shards(mesh.shape["row"], mesh.shape["col"], *arrays)

    return jax.shard_map(
        body, mesh=mesh, in_specs=placed, out_specs=P("row", "col"), check_vma=False
    )
```
